32 devices in a mesh: groups: 2 (over y), chan: 8 (over z, x), sub: 2 (over core).
Axes of the slice: x: 2, y: 2, z: 4, core: 2. Of those that a mesh axis runs over, the one named last changes fastest.
Arguments:
- predicted_sky_response: bfloat16 [16384, 8, 2, 128], P(('groups', 'chan', 'sub')), parts along dimension 0, may hold values from -0.4375 to 0.4375
- measured_correlation: bfloat16 [16384, 2, 128], P(('groups', 'chan', 'sub')), parts along dimension 0, may hold values from -6 to 6
- keep_indicator: int32 [16384, 128], P(('groups', 'chan', 'sub')), parts along dimension 0, may hold values 0 or 1
- tile_owner: int32 [16384, 1], P(('groups', 'chan', 'sub')), parts along dimension 0, may hold values from 0 to 7; in each aligned block of 512 rows (0 to 511, 512 to 1023, ...) at most 192 rows name the same one
- tile_channel: int32 [16384], P(('groups', 'chan', 'sub')), parts along dimension 0, may hold values from 0 to 3
- tile_base: int32 [16384], P(('groups', 'chan', 'sub')), parts along dimension 0, may hold values from 0 to 14
- pairs: int32 [15, 2, 128], replicated, may hold values from 0 to 61, as said below
- gains: float32 [64, 2, 62, 8], P(('groups', 'chan')), parts along dimension 0, may hold values from -5 to 5
- duals: float32 [64, 2, 62, 8], P(('groups', 'chan', 'sub')), parts along dimension 0, may hold values from -4 to 4
- consensus: float32 [8, 2, 62, 8], P('groups'), parts along dimension 0, may hold values from -5 to 5
- rho: float32 [8], replicated, may hold values from 0.3 to 3
Outputs:
- gains_new: float32 [64, 2, 62, 8], P(('groups', 'chan', 'sub')), parts along dimension 0
- consensus_new: float32 [8, 2, 62, 8], P('groups'), parts along dimension 0
- duals_new: float32 [64, 2, 62, 8], P(('groups', 'chan', 'sub')), parts along dimension 0
The draws below stay inside these ranges and needn't reach their ends.
There are 2 independent parts, one for each index of `groups`. The reference program is written for one: setup_inputs(seed, part) draws one part's arguments, and reference() takes and returns one part's arrays. A program takes and returns all parts, laid end to end along the dimension named above; an argument that names none is the same for every part. Nothing has to cross between parts.
Inputs may be any that keep to these rules, and one draw needn't show every extreme that they name: `tile_owner`: on the tiles of one device at most 192 name the same owner, a bound that some block reaches. `pairs`: the two stations of a row differ.
All inputs are finite; a program needn't handle non-finite values. No bound on the sum of `keep_indicator` on one device may be relied on, other than what follows from the above.
Results may differ from the reference program's by a relative error of at most 0.0027.
Values may be sent and summed in bfloat16 or wider, within the bound.
A program may use at most 128 MiB of HBM per device.

```python
import math
import jax
import jax.numpy as jnp
import numpy as np
from jax import lax

NS = 62
K = 8
DEG = 4
TR = 128
BT = 15
CH_DEV = 4
TILES_DEV = 512
F = 32
TILES = 8192
CAP = 192
ROWS_CH = 32768
N_CHAN = 8


def draw_pairs(key, part):
    key_first, key_offset = jax.random.split(jax.random.fold_in(key, 17))
    first_station = jax.random.randint(key_first, (BT, TR), 0, NS)
    offset = jax.random.randint(key_offset, (BT, TR), 1, NS)
    station_second = (first_station + offset) % NS
    return jnp.stack([first_station, station_second], axis=1).astype(jnp.int32)


def touch_ends(result, own_key, smallest, top_value):
    longest = result.shape.index(max(result.shape))
    spots = []
    for shift in (0, 1):
        where = [jax.random.randint(jax.random.fold_in(own_key, axis), (), 0, length) for axis, length in enumerate(result.shape)]
        where[longest] = (where[longest] + shift) % result.shape[longest]
        spots.append(tuple(where))
    return result.at[spots[0]].set(smallest).at[spots[1]].set(top_value)


def block_scale(rng, extent, pieces, low, top_value):
    factor_of, own = 1.0, jax.random.fold_in(rng, 6)
    for position, blocks in pieces:
        steps = jnp.exp(jax.random.uniform(jax.random.fold_in(own, position), (blocks,), jnp.float32, low / len(pieces), top_value / len(pieces)))
        factor_of = factor_of * jnp.repeat(steps, extent[position] // blocks).reshape([-1 if axis == position else 1 for axis in range(len(extent))])
    return factor_of


def assign_block(own_key, own, number, rows, number_of, top, bound, skew):
    order = jax.random.permutation(own_key, number_of)
    heavy_load, common = load_shares(number_of, rows * top, bound, skew, True), load_shares(number_of, rows * top, bound, skew, False)
    places = jnp.arange(number_of)

    def named(tallies, rotation):
        used = int((tallies > 0).sum())
        fixed = max(1, used // 4)
        passed = fixed + (places - fixed + rotation * (used - fixed)) % max(1, number_of - fixed)
        return jnp.zeros((number_of,), jnp.int32).at[order[jnp.where(places < fixed, places, passed)]].set(jnp.asarray(tallies, jnp.int32))

    tallies = jnp.where(number % 4 == 0, named(heavy_load, number // 4), named(common, number - number // 4 - 1))
    mixed = jax.random.permutation(jax.random.fold_in(own, 3), number_of)
    giver, taker = mixed[0:number_of // 2 * 2:2], mixed[1:number_of // 2 * 2:2]
    room = jnp.minimum(tallies[giver] - 1, bound - tallies[taker]) // 2
    room = jnp.where((giver == order[0]) | (taker == order[0]) | (tallies[taker] == 0), 0, jnp.maximum(room, 0))
    passed = jax.random.randint(jax.random.fold_in(own, 4), (number_of // 2,), 0, 1 << 20) % (room + 1)
    tallies = tallies.at[giver].add(-passed).at[taker].add(passed)
    members = jnp.searchsorted(jnp.cumsum(tallies), jnp.arange(rows * top), side="right").astype(jnp.int32)
    table = members.reshape(top, rows).T
    table = table[jax.random.permutation(jax.random.fold_in(own, 1), rows)]
    rotation = jax.random.randint(jax.random.fold_in(own, 2), (rows, 1), 0, top)
    return jnp.take_along_axis(table, (jnp.arange(top)[None, :] + rotation) % top, axis=1)


def load_shares(count, total, most, skew, full):
    loads = [(1 << 20) // math.isqrt(grade ** skew) + 1 for grade in range(1, count + 1)]
    largest = most if full else min(most, max(-(-total // count), total * loads[0] // sum(loads)))
    least = 1 if total - largest >= count - 1 else 0
    given, rest = [largest] + [least] * (count - 1), total - largest - least * (count - 1)
    while rest > 0:
        movable = [i for i in range(1, count) if given[i] < largest] or [i for i in range(1, count) if given[i] < most]
        mass, remaining = sum([loads[i] for i in movable]), rest
        for i in movable:
            more = min(most - given[i], max(1, remaining * loads[i] // mass), rest)
            given[i] = given[i] + more
            rest = rest - more
    return np.array(given)


def scatter_about(key, shape, width, most, shards=(), kind=jnp.bfloat16):
    result = jax.random.normal(key, shape, jnp.float32) * width
    if len(shards) > 0:
        result = block_scale(key, shape, shards, -0.22, 0.18) * result
    return jnp.clip(result, min=-most, max=most).astype(kind)


def setup_inputs(seed: int = 0, part: int = 0) -> dict:
    arg_keys = jax.random.split(jax.random.key(seed), 12)
    own_keys = jax.random.split(jax.random.fold_in(arg_keys[11], part), 12)
    predicted_sky_response = scatter_about(own_keys[0], (TILES, K, 2, TR), ((2 * ROWS_CH // NS) ** -0.5), 0.4375, ((0, 16),))
    measured_correlation = scatter_about(own_keys[1], (TILES, 2, TR), 1.0, 6.0, ((0, 16),))
    keep_indicator = touch_ends((jax.random.randint(own_keys[2], (TILES, TR), 0, 4) < 3).astype(jnp.int32), jax.random.fold_in(own_keys[2], 1), 0, 1)
    tile_owner_keys = jax.random.split(jax.random.fold_in(own_keys[3], 1), TILES // TILES_DEV)
    tile_owner_turns = jax.random.permutation(jax.random.fold_in(own_keys[3], 3), TILES // TILES_DEV)
    tile_owner = jax.vmap(lambda own, number: assign_block(jax.random.fold_in(own_keys[3], 2), own, number, TILES_DEV, N_CHAN, 1, CAP, 2))(tile_owner_keys, tile_owner_turns).reshape((TILES, 1))
    tile_channel = touch_ends(jax.random.randint(own_keys[4], (TILES,), 0, CH_DEV), jax.random.fold_in(own_keys[4], 1), 0, CH_DEV - 1).astype(jnp.int32)
    tile_base = touch_ends(jax.random.randint(own_keys[5], (TILES,), 0, BT), jax.random.fold_in(own_keys[5], 1), 0, BT - 1).astype(jnp.int32)
    pairs = draw_pairs(jax.random.fold_in(arg_keys[11], 71), part)
    gains = scatter_about(own_keys[7], (F, 2, NS, K), 0.8, 5.0, ((0, 8),), jnp.float32)
    duals = scatter_about(own_keys[8], (F, 2, NS, K), 0.3, 4.0, ((0, 16),), jnp.float32)
    consensus = scatter_about(own_keys[9], (DEG, 2, NS, K), 0.5, 5.0, (), jnp.float32)
    rho = jnp.clip(jnp.exp(jax.random.uniform(arg_keys[10], (K,), jnp.float32, math.log(0.3), math.log(3.0))), 0.3, 3.0)
    return dict(predicted_sky_response=predicted_sky_response, measured_correlation=measured_correlation, keep_indicator=keep_indicator, tile_owner=tile_owner, tile_channel=tile_channel, tile_base=tile_base, pairs=pairs, gains=gains, duals=duals, consensus=consensus, rho=rho)


def legendre_rows(channels):
    positions = jnp.arange(channels, dtype=jnp.float32)
    abscissa = (2.0 * positions - (channels - 1)) / max(channels - 1, 1)
    return jnp.stack([jnp.ones_like(abscissa), abscissa, 0.5 * (3.0 * abscissa * abscissa - 1.0), 0.5 * (5.0 * abscissa * abscissa * abscissa - 3.0 * abscissa)])

def outer_terms(vector_real, vector_imag, weight_real, weight_imag):
    tiles_count, row_total_count, directions = vector_real.shape
    outer_real = vector_real[..., :, None] * vector_real[..., None, :] + vector_imag[..., :, None] * vector_imag[..., None, :]
    outer_imag = vector_real[..., :, None] * vector_imag[..., None, :] - vector_imag[..., :, None] * vector_real[..., None, :]
    normal = jnp.stack([outer_real, outer_imag], axis=2).reshape(tiles_count, row_total_count, 2 * directions * directions)
    side_real = vector_real * weight_real[..., None] + vector_imag * weight_imag[..., None]
    side_imag = vector_real * weight_imag[..., None] - vector_imag * weight_real[..., None]
    right_side = jnp.stack([side_real, side_imag], axis=2).reshape(tiles_count, row_total_count, 2 * directions)
    return (normal, right_side)

def row_terms(coupling, observed, near_gain, far_gain):
    coupling_real = jnp.swapaxes(coupling[:, :, 0, :], 1, 2).astype(jnp.float32)
    coupling_imag = jnp.swapaxes(coupling[:, :, 1, :], 1, 2).astype(jnp.float32)
    near_real, near_imag = (near_gain[:, :, 0, :], near_gain[:, :, 1, :])
    far_real, far_imag = (far_gain[:, :, 0, :], far_gain[:, :, 1, :])
    slope_real = coupling_real * far_real + coupling_imag * far_imag
    slope_imag = coupling_imag * far_real - coupling_real * far_imag
    mirror_real = coupling_real * near_real - coupling_imag * near_imag
    mirror_imag = -(coupling_real * near_imag + coupling_imag * near_real)
    model_real = jnp.sum(near_real * slope_real - near_imag * slope_imag, axis=-1)
    model_imag = jnp.sum(near_real * slope_imag + near_imag * slope_real, axis=-1)
    observed_f = observed.astype(jnp.float32)
    residual_real = observed_f[:, 0, :] - model_real
    residual_imag = observed_f[:, 1, :] - model_imag
    normal_near, right_near = outer_terms(slope_real, slope_imag, residual_real, residual_imag)
    normal_far, right_far = outer_terms(mirror_real, mirror_imag, residual_real, -residual_imag)
    normal = jnp.concatenate([normal_near, normal_far], axis=1).astype(jnp.bfloat16)
    right_side = jnp.concatenate([right_near, right_far], axis=1).astype(jnp.bfloat16)
    return (normal, right_side)

def admm_update(normal, right_side, gain, dual, anchor, rho):
    count, stations = (normal.shape[0], normal.shape[1])
    directions = rho.shape[0]
    normal_blocks = normal.reshape(count, stations, 2, directions, directions)
    ridge_diag = jnp.diag(rho)
    higher_half_records = jnp.concatenate([normal_blocks[:, :, 0] + ridge_diag, -normal_blocks[:, :, 1]], axis=-1)
    lower_rows = jnp.concatenate([normal_blocks[:, :, 1], normal_blocks[:, :, 0] + ridge_diag], axis=-1)
    system = jnp.concatenate([higher_half_records, lower_rows], axis=-2)
    gain_rows = jnp.transpose(gain, (0, 2, 1, 3))
    dual_rows = jnp.transpose(dual, (0, 2, 1, 3))
    anchor_rows = jnp.transpose(anchor, (0, 2, 1, 3))
    target = right_side.reshape(count, stations, 2, directions) - dual_rows - rho * (gain_rows - anchor_rows)
    factor = jnp.linalg.cholesky(system)
    gain_step = jax.scipy.linalg.cho_solve((factor, True), target.reshape(count, stations, 2 * directions)[..., None])[..., 0]
    return gain + jnp.transpose(gain_step.reshape(count, stations, 2, directions), (0, 2, 1, 3))

def fit_consensus(poly_basis, summed):
    gram_matrix = jnp.dot(poly_basis, poly_basis.T, precision=lax.Precision.HIGHEST)
    factor = jnp.linalg.cholesky(gram_matrix)
    coeffs = jax.scipy.linalg.cho_solve((factor, True), summed.reshape(summed.shape[0], -1))
    return coeffs.reshape(summed.shape)

def reference(predicted_sky_response, measured_correlation, keep_indicator, tile_owner, tile_channel, tile_base, pairs, gains, duals, consensus, rho):
    channels = CH_DEV * N_CHAN
    retained_selector = keep_indicator > 0
    predicted_response_kept = jnp.where(retained_selector[:, None, None, :], predicted_sky_response, jnp.zeros_like(predicted_sky_response))
    measured_correlation_kept = jnp.where(retained_selector[:, None, :], measured_correlation, jnp.zeros_like(measured_correlation))
    channel_lookup = (tile_owner[:, 0] * CH_DEV + tile_channel).astype(jnp.int32)
    gain_table = jnp.transpose(gains, (0, 2, 1, 3))
    iteration_tally = predicted_sky_response.shape[0] // TILES_DEV
    normal_matrix_width = 2 * K * K

    def one_block(totals, block_item):
        normal_acc, right_acc = totals
        block_coherency, block_visibility, block_channel, block_base = block_item
        stations = pairs[block_base]
        first_station = stations[:, 0, :]
        station_second = stations[:, 1, :]
        near_gain = gain_table[block_channel[:, None], first_station]
        far_gain = gain_table[block_channel[:, None], station_second]
        normal, right_side = row_terms(block_coherency, block_visibility, near_gain, far_gain)
        normal = lax.optimization_barrier(normal).astype(jnp.float32)
        right_side = lax.optimization_barrier(right_side).astype(jnp.float32)
        segment_ids = (jnp.concatenate([first_station, station_second], axis=1) + block_channel[:, None] * NS).astype(jnp.int32)
        normal_acc = normal_acc + jax.ops.segment_sum(normal.reshape(-1, normal_matrix_width), segment_ids.reshape(-1), num_segments=channels * NS)
        right_acc = right_acc + jax.ops.segment_sum(right_side.reshape(-1, 2 * K), segment_ids.reshape(-1), num_segments=channels * NS)
        return ((normal_acc, right_acc), None)
    block_items = (predicted_response_kept.reshape((iteration_tally, TILES_DEV) + predicted_sky_response.shape[1:]), measured_correlation_kept.reshape((iteration_tally, TILES_DEV) + measured_correlation.shape[1:]), channel_lookup.reshape(iteration_tally, TILES_DEV), tile_base.reshape(iteration_tally, TILES_DEV))
    start_totals = (jnp.zeros((channels * NS, normal_matrix_width), jnp.float32), jnp.zeros((channels * NS, 2 * K), jnp.float32))
    (normal_sum, right_sum), _ = lax.scan(one_block, start_totals, block_items)
    normal_sum = normal_sum.reshape(channels, NS, normal_matrix_width)
    right_sum = right_sum.reshape(channels, NS, 2 * K)
    poly_basis = legendre_rows(channels)
    anchor = jnp.einsum('df,dcsk->fcsk', poly_basis, consensus, precision=lax.Precision.HIGHEST)
    gains_new = admm_update(normal_sum, right_sum, gains, duals, anchor, rho)
    summed = jnp.einsum('df,fcsk->dcsk', poly_basis, gains_new + duals / rho, precision=lax.Precision.HIGHEST)
    consensus_new = fit_consensus(poly_basis, summed)
    duals_new = duals + rho * (gains_new - jnp.einsum('df,dcsk->fcsk', poly_basis, consensus_new, precision=lax.Precision.HIGHEST))
    return (gains_new, consensus_new, duals_new)
```

```python
import functools

import jax
import jax.numpy as jnp
from jax import lax
from jax.experimental import pallas as pl
from jax.experimental.pallas import tpu as pltpu
from jax.sharding import PartitionSpec as P

LANES = 128


def legendre_rows(channels):
    positions = jnp.arange(channels, dtype=jnp.float32)
    abscissa = (2.0 * positions - (channels - 1)) / max(channels - 1, 1)
    return jnp.stack(
        [
            jnp.ones_like(abscissa),
            abscissa,
            0.5 * (3.0 * abscissa * abscissa - 1.0),
            0.5 * (5.0 * abscissa * abscissa * abscissa - 3.0 * abscissa),
        ]
    )


def hermitian_rows(real, imag, upper):
    half = real.shape[0] // 2
    groups_real = [real * real + imag * imag]
    groups_imag = []
    for shift in range(1, half + 1):
        turned_real = pltpu.roll(real, 2 * half - shift, axis=0)
        turned_imag = pltpu.roll(imag, 2 * half - shift, axis=0)
        groups_real.append(real * turned_real + imag * turned_imag)
        groups_imag.append(real * turned_imag - imag * turned_real)
    mixed = jnp.where(upper, groups_real.pop(), groups_imag.pop())
    return groups_real + groups_imag + [mixed]


def accumulate_kernel(
    block,
    unroll,
    half,
    stations,
    channel_ref,
    base_ref,
    coupling_ref,
    observed_ref,
    keep_ref,
    pairs_ref,
    gains_ref,
    out_ref,
    table,
    turned,
    coupling_f,
    observed_f,
    keep_f,
):
    step = pl.program_id(0)
    bases = pairs_ref.shape[0] // 2
    tile_rows = keep_ref.shape[1]
    width = LANES // half
    directions = gains_ref.shape[1]

    @pl.when(step == 0)
    def _():
        out_ref[...] = jnp.zeros_like(out_ref)
        turned[...] = jnp.zeros_like(turned)
        turned[: 2 * bases, :] = pairs_ref[...].astype(jnp.float32)
        columns = jnp.transpose(turned[...])
        lane = lax.broadcasted_iota(jnp.int32, (tile_rows, LANES), 1).astype(jnp.float32)
        for base in range(bases):
            for end in range(2):
                station = columns[:, 2 * base + end : 2 * base + end + 1]
                for part in range(half):
                    table[base * half + part, end * tile_rows : (end + 1) * tile_rows, :] = (
                        jnp.where(station + float(part * width) == lane, 1.0, 0.0).astype(jnp.bfloat16)
                    )

    coupling_f[...] = coupling_ref[...].astype(jnp.float32)
    observed_f[...] = observed_ref[...].astype(jnp.float32)
    keep_f[...] = jnp.where(keep_ref[...] > 0, 1.0, 0.0)
    upper = lax.broadcasted_iota(jnp.int32, (directions, LANES), 0) < directions // 2

    def spread(row):
        return jnp.broadcast_to(row, (directions, LANES))

    def one_tile(local):
        tile = step * block + local
        channel = channel_ref[tile]
        base = base_ref[tile]
        kept = spread(keep_f[pl.ds(local, 1), :])
        first = local * 2 * directions
        real = coupling_f[pl.ds(first, directions, stride=2), :] * kept
        imag = coupling_f[pl.ds(first + 1, directions, stride=2), :] * kept
        seen_real = spread(observed_f[pl.ds(2 * local, 1), :])
        seen_imag = spread(observed_f[pl.ds(2 * local + 1, 1), :])
        near = spread(pairs_ref[pl.ds(2 * base, 1), :])
        far = spread(pairs_ref[pl.ds(2 * base + 1, 1), :])
        gain_real = gains_ref[2 * channel]
        gain_imag = gains_ref[2 * channel + 1]

        def pick(values, index):
            return jnp.take_along_axis(values, index, axis=1, mode="promise_in_bounds")

        near_real, near_imag = pick(gain_real, near), pick(gain_imag, near)
        far_real, far_imag = pick(gain_real, far), pick(gain_imag, far)
        slope_real = real * far_real + imag * far_imag
        slope_imag = imag * far_real - real * far_imag
        mirror_real = real * near_real - imag * near_imag
        mirror_imag = -(real * near_imag + imag * near_real)

        def end_rows(vector_real, vector_imag, weight_real, weight_imag):
            side_real = vector_real * weight_real + vector_imag * weight_imag
            side_imag = vector_real * weight_imag - vector_imag * weight_real
            groups = hermitian_rows(vector_real, vector_imag, upper)
            whole = jnp.concatenate(groups, axis=0).astype(jnp.bfloat16)
            side = jnp.concatenate([side_real, side_imag], axis=0)
            high = side.astype(jnp.bfloat16)
            low = (side - high.astype(jnp.float32)).astype(jnp.bfloat16)
            return jnp.concatenate([whole, high, low], axis=0)

        rows = jnp.concatenate(
            [
                end_rows(slope_real, slope_imag, seen_real, seen_imag),
                end_rows(mirror_real, mirror_imag, seen_real, -seen_imag),
            ],
            axis=1,
        )
        place = lax.rem(channel, half)
        sums = jnp.dot(rows, table[base * half + place], preferred_element_type=jnp.float32)
        normal_rows = directions * directions
        return lax.div(channel, half), jnp.concatenate(
            [
                sums[:normal_rows],
                sums[normal_rows : normal_rows + 2 * directions] + sums[normal_rows + 2 * directions :],
            ],
            axis=0,
        )

    def one_group(group, carry):
        results = [one_tile(group * unroll + number) for number in range(unroll)]
        for owner, sums in results:
            out_ref[owner] += sums
        return carry

    lax.fori_loop(0, block // unroll, one_group, 0)


def accumulate(coupling, observed, keep, channel, base, pairs, gain_table, half, stations):
    tiles, directions, _, tile_rows = coupling.shape
    channels = gain_table.shape[0] // 2
    bases = pairs.shape[0]
    block = min(64, tiles)
    unroll = 8
    kernel = functools.partial(accumulate_kernel, block, unroll, half, stations)
    out_rows = directions * directions + 2 * directions
    return pl.pallas_call(
        kernel,
        grid_spec=pltpu.PrefetchScalarGridSpec(
            num_scalar_prefetch=2,
            grid=(tiles // block,),
            in_specs=[
                pl.BlockSpec((block * 2 * directions, tile_rows), lambda i, *_: (i, 0)),
                pl.BlockSpec((block * 2, tile_rows), lambda i, *_: (i, 0)),
                pl.BlockSpec((block, tile_rows), lambda i, *_: (i, 0)),
                pl.BlockSpec((2 * bases, tile_rows), lambda i, *_: (0, 0)),
                pl.BlockSpec(gain_table.shape, lambda i, *_: (0, 0, 0)),
            ],
            out_specs=pl.BlockSpec(
                (channels // half, out_rows, LANES), lambda i, *_: (0, 0, 0)
            ),
            scratch_shapes=[
                pltpu.VMEM((bases * half, 2 * tile_rows, LANES), jnp.bfloat16),
                pltpu.VMEM((LANES, tile_rows), jnp.float32),
                pltpu.VMEM((block * 2 * directions, tile_rows), jnp.float32),
                pltpu.VMEM((block * 2, tile_rows), jnp.float32),
                pltpu.VMEM((block, tile_rows), jnp.float32),
            ],
        ),
        out_shape=jax.ShapeDtypeStruct((channels // half, out_rows, LANES), jnp.float32),
        compiler_params=pltpu.CompilerParams(
            dimension_semantics=("arbitrary",), vmem_limit_bytes=60 << 20
        ),
    )(
        channel,
        base,
        coupling.reshape(tiles * 2 * directions, tile_rows),
        observed.reshape(tiles * 2, tile_rows),
        keep,
        pairs.reshape(2 * bases, tile_rows),
        gain_table,
    )


def unpack_normal(packed, directions):
    half = directions // 2
    groups = packed[: directions * directions].reshape(directions, directions, -1)
    mixed = groups[-1]
    real = [groups[d] for d in range(half)]
    imag = [jnp.zeros_like(groups[0])] + [groups[half + d] for d in range(half - 1)]
    real.append(jnp.concatenate([mixed[:half], mixed[:half]], axis=0))
    imag.append(jnp.concatenate([-mixed[half:], mixed[half:]], axis=0))
    out_real, out_imag = [], []
    for k in range(directions):
        row_real, row_imag = [], []
        for l in range(directions):
            d = (l - k) % directions
            if d <= half:
                row_real.append(real[d][k])
                row_imag.append(imag[d][k])
            else:
                row_real.append(real[directions - d][l])
                row_imag.append(-imag[directions - d][l])
        out_real.append(jnp.stack(row_real))
        out_imag.append(jnp.stack(row_imag))
    return jnp.stack(out_real), jnp.stack(out_imag)


def fit_consensus(poly_basis, summed):
    gram_matrix = jnp.dot(poly_basis, poly_basis.T, precision=lax.Precision.HIGHEST)
    factor = jnp.linalg.cholesky(gram_matrix)
    coeffs = jax.scipy.linalg.cho_solve((factor, True), summed.reshape(summed.shape[0], -1))
    return coeffs.reshape(summed.shape)


def body(
    predicted_sky_response,
    measured_correlation,
    keep_indicator,
    tile_owner,
    tile_channel,
    tile_base,
    pairs,
    gains,
    duals,
    consensus,
    rho,
):
    channels_here, _, stations, directions = gains.shape
    chan_count = lax.axis_size("chan")
    sub_count = lax.axis_size("sub")
    half = channels_here // sub_count
    turned = jnp.swapaxes(gains, 2, 3)
    turned = jnp.pad(turned, ((0, 0), (0, 0), (0, 0), (0, LANES - stations)))
    all_gains = lax.all_gather(turned, "chan", axis=0, tiled=True)
    full_channel = tile_owner[:, 0] * channels_here + tile_channel
    packed = accumulate(
        predicted_sky_response,
        measured_correlation,
        keep_indicator,
        full_channel,
        tile_base,
        pairs,
        all_gains.reshape(-1, directions, LANES),
        half,
        stations,
    )
    mine = lax.psum_scatter(packed, ("chan", "sub"), scatter_dimension=0, tiled=True)[0]
    sub_index = lax.axis_index("sub")
    chan_index = lax.axis_index("chan")
    poly_basis = legendre_rows(channels_here * chan_count)
    first_channel = (chan_index * sub_count + sub_index) * half
    my_basis = lax.dynamic_slice_in_dim(poly_basis, first_channel, half, 1)
    anchor = jnp.einsum("df,dcsk->fcsk", my_basis, consensus, precision=lax.Precision.HIGHEST)
    real, imag = unpack_normal(mine, directions)
    width = LANES // half

    def by_station(x):
        x = x.reshape(x.shape[:-1] + (half, width))[..., :stations]
        return jnp.moveaxis(x, (-2, -1), (0, 1))

    real, imag = by_station(real), by_station(imag)
    ridge = jnp.diag(rho)
    system = jnp.concatenate(
        [
            jnp.concatenate([real + ridge, -imag], axis=-1),
            jnp.concatenate([imag, real + ridge], axis=-1),
        ],
        axis=-2,
    )
    side = by_station(mine[directions * directions :].reshape(2, directions, LANES))
    duals_rows = jnp.transpose(duals, (0, 2, 1, 3))
    anchor_rows = jnp.transpose(anchor, (0, 2, 1, 3))
    target = side - duals_rows + rho * anchor_rows
    factor = jnp.linalg.cholesky(system)
    solved = jax.scipy.linalg.cho_solve(
        (factor, True), target.reshape(half, stations, 2 * directions)[..., None]
    )[..., 0]
    gains_new = jnp.transpose(solved.reshape(half, stations, 2, directions), (0, 2, 1, 3))
    partial_value = jnp.einsum(
        "df,fcsk->dcsk", my_basis, gains_new + duals / rho, precision=lax.Precision.HIGHEST
    )
    summed = lax.psum(partial_value, ("chan", "sub"))
    consensus_new = fit_consensus(poly_basis, summed)
    duals_new = duals + rho * (
        gains_new
        - jnp.einsum("df,dcsk->fcsk", my_basis, consensus_new, precision=lax.Precision.HIGHEST)
    )
    return (gains_new, consensus_new, duals_new)


def solution(mesh):
    placed = (
        P(("groups", "chan", "sub"), None, None, None),
        P(("groups", "chan", "sub"), None, None),
        P(("groups", "chan", "sub"), None),
        P(("groups", "chan", "sub"), None),
        P(("groups", "chan", "sub")),
        P(("groups", "chan", "sub")),
        P(),
        P(("groups", "chan"), None, None, None),
        P(("groups", "chan", "sub"), None, None, None),
        P("groups", None, None, None),
        P(),
    )
    return jax.shard_map(
        body,
        mesh=mesh,
        in_specs=placed,
        out_specs=(
            P(("groups", "chan", "sub"), None, None, None),
            P("groups", None, None, None),
            P(("groups", "chan", "sub"), None, None, None),
        ),
        check_vma=False,
    )
```

```python
import functools

import jax
import jax.numpy as jnp
import numpy as np
from jax import lax
from jax.experimental import pallas as pl
from jax.experimental.pallas import tpu as pltpu
from jax.sharding import PartitionSpec as P

LANES = 128


def hermitian_rows(real, imag, upper):
    half = real.shape[0] // 2
    groups_real = [real * real + imag * imag]
    groups_imag = []
    for shift in range(1, half + 1):
        turned_real = pltpu.roll(real, 2 * half - shift, axis=0)
        turned_imag = pltpu.roll(imag, 2 * half - shift, axis=0)
        groups_real.append(real * turned_real + imag * turned_imag)
        groups_imag.append(real * turned_imag - imag * turned_real)
    mixed = jnp.where(upper, groups_real.pop(), groups_imag.pop())
    return groups_real + groups_imag + [mixed]


def accumulate_kernel(
    block,
    unroll,
    half,
    channel_ref,
    base_ref,
    coupling_ref,
    observed_ref,
    keep_ref,
    pairs_ref,
    gains_ref,
    out_ref,
    table,
    turned,
    coupling_f,
    observed_f,
    keep_f,
):
    step = pl.program_id(0)
    bases = pairs_ref.shape[0] // 2
    tile_rows = keep_ref.shape[1]
    width = LANES // half
    directions = gains_ref.shape[1]

    @pl.when(step == 0)
    def _():
        out_ref[...] = jnp.zeros_like(out_ref)
        turned[...] = jnp.zeros_like(turned)
        turned[: 2 * bases, :] = pairs_ref[...].astype(jnp.float32)
        columns = jnp.transpose(turned[...])
        lane = lax.broadcasted_iota(jnp.int32, (tile_rows, LANES), 1).astype(jnp.float32)
        for base in range(bases):
            for end in range(2):
                station = columns[:, 2 * base + end : 2 * base + end + 1]
                for part in range(half):
                    table[base * half + part, end * tile_rows : (end + 1) * tile_rows, :] = (
                        jnp.where(station + float(part * width) == lane, 1.0, 0.0).astype(jnp.bfloat16)
                    )

    coupling_f[...] = coupling_ref[...].astype(jnp.float32)
    observed_f[...] = observed_ref[...].astype(jnp.float32)
    keep_f[...] = jnp.where(keep_ref[...] > 0, 1.0, 0.0)
    upper = lax.broadcasted_iota(jnp.int32, (directions, LANES), 0) < directions // 2

    def spread(row):
        return jnp.broadcast_to(row, (directions, LANES))

    def one_tile(local):
        tile = step * block + local
        channel = channel_ref[tile]
        base = base_ref[tile]
        kept = spread(keep_f[pl.ds(local, 1), :])
        first = local * 2 * directions
        real = coupling_f[pl.ds(first, directions, stride=2), :] * kept
        imag = coupling_f[pl.ds(first + 1, directions, stride=2), :] * kept
        seen_real = spread(observed_f[pl.ds(2 * local, 1), :])
        seen_imag = spread(observed_f[pl.ds(2 * local + 1, 1), :])
        near = spread(pairs_ref[pl.ds(2 * base, 1), :])
        far = spread(pairs_ref[pl.ds(2 * base + 1, 1), :])
        place = lax.rem(channel, half)
        owner = lax.div(channel, half)
        near, far = near + place * width, far + place * width
        gain_real = gains_ref[2 * owner]
        gain_imag = gains_ref[2 * owner + 1]

        def pick(values, index):
            return jnp.take_along_axis(values, index, axis=1, mode="promise_in_bounds")

        near_real, near_imag = pick(gain_real, near), pick(gain_imag, near)
        far_real, far_imag = pick(gain_real, far), pick(gain_imag, far)
        slope_real = real * far_real + imag * far_imag
        slope_imag = imag * far_real - real * far_imag
        mirror_real = real * near_real - imag * near_imag
        mirror_imag = -(real * near_imag + imag * near_real)

        def end_rows(vector_real, vector_imag, weight_real, weight_imag):
            side_real = vector_real * weight_real + vector_imag * weight_imag
            side_imag = vector_real * weight_imag - vector_imag * weight_real
            groups = hermitian_rows(vector_real, vector_imag, upper)
            whole = jnp.concatenate(groups, axis=0).astype(jnp.bfloat16)
            side = jnp.concatenate([side_real, side_imag], axis=0)
            high = side.astype(jnp.bfloat16)
            low = (side - high.astype(jnp.float32)).astype(jnp.bfloat16)
            return jnp.concatenate([whole, high, low], axis=0)

        rows = jnp.concatenate(
            [
                end_rows(slope_real, slope_imag, seen_real, seen_imag),
                end_rows(mirror_real, mirror_imag, seen_real, -seen_imag),
            ],
            axis=1,
        )
        sums = jnp.dot(rows, table[base * half + place], preferred_element_type=jnp.float32)
        normal_rows = directions * directions
        return owner, jnp.concatenate(
            [
                sums[:normal_rows],
                sums[normal_rows : normal_rows + 2 * directions] + sums[normal_rows + 2 * directions :],
            ],
            axis=0,
        )

    def one_group(group, carry):
        results = [one_tile(group * unroll + number) for number in range(unroll)]
        for owner, sums in results:
            out_ref[owner] += sums
        return carry

    lax.fori_loop(0, block // unroll, one_group, 0)


def accumulate(coupling, observed, keep, channel, base, pairs, gain_table, half):
    tiles, directions, _, tile_rows = coupling.shape
    owners = gain_table.shape[0] // 2
    bases = pairs.shape[0]
    block = min(64, tiles)
    unroll = 8
    kernel = functools.partial(accumulate_kernel, block, unroll, half)
    out_rows = directions * directions + 2 * directions
    return pl.pallas_call(
        kernel,
        grid_spec=pltpu.PrefetchScalarGridSpec(
            num_scalar_prefetch=2,
            grid=(tiles // block,),
            in_specs=[
                pl.BlockSpec((block * 2 * directions, tile_rows), lambda i, *_: (i, 0)),
                pl.BlockSpec((block * 2, tile_rows), lambda i, *_: (i, 0)),
                pl.BlockSpec((block, tile_rows), lambda i, *_: (i, 0)),
                pl.BlockSpec((2 * bases, tile_rows), lambda i, *_: (0, 0)),
                pl.BlockSpec(gain_table.shape, lambda i, *_: (0, 0, 0)),
            ],
            out_specs=pl.BlockSpec(
                (owners, out_rows, LANES), lambda i, *_: (0, 0, 0)
            ),
            scratch_shapes=[
                pltpu.VMEM((bases * half, 2 * tile_rows, LANES), jnp.bfloat16),
                pltpu.VMEM((LANES, tile_rows), jnp.float32),
                pltpu.VMEM((block * 2 * directions, tile_rows), jnp.float32),
                pltpu.VMEM((block * 2, tile_rows), jnp.float32),
                pltpu.VMEM((block, tile_rows), jnp.float32),
            ],
        ),
        out_shape=jax.ShapeDtypeStruct((owners, out_rows, LANES), jnp.float32),
        compiler_params=pltpu.CompilerParams(
            dimension_semantics=("arbitrary",), vmem_limit_bytes=60 << 20
        ),
    )(
        channel,
        base,
        coupling.reshape(tiles * 2 * directions, tile_rows),
        observed.reshape(tiles * 2, tile_rows),
        keep,
        pairs.reshape(2 * bases, tile_rows),
        gain_table,
    )


def lay_pair(load, pad, half, width):
    total = None
    for part in range(half):
        block = load(part)
        pad[part % 2, :, : block.shape[1]] = block
        value = pad[part % 2]
        if part:
            value = pltpu.roll(value, part * width, axis=1)
        total = value if total is None else total + value
    return total


def gather_kernel(chan_count, sub_count, half, gains_ref, out_ref, pad, send_sem, recv_sem):
    chan = lax.axis_index("chan")
    width = LANES // half
    pad[...] = jnp.zeros_like(pad)
    for owner in range(sub_count):
        for part in range(2):
            out_ref[chan, owner, part] = lay_pair(
                lambda number: gains_ref[owner * half + number, part], pad, half, width
            )
    barrier = pltpu.get_barrier_semaphore()
    for offset in range(1, chan_count):
        pl.semaphore_signal(
            barrier,
            inc=1,
            device_id={"chan": lax.rem(chan + offset, chan_count)},
            device_id_type=pl.DeviceIdType.MESH,
        )
    pl.semaphore_wait(barrier, chan_count - 1)
    copies = []
    for offset in range(1, chan_count):
        copy = pltpu.make_async_remote_copy(
            src_ref=out_ref.at[chan],
            dst_ref=out_ref.at[chan],
            send_sem=send_sem.at[offset],
            recv_sem=recv_sem.at[offset],
            device_id={"chan": lax.rem(chan + offset, chan_count)},
            device_id_type=pl.DeviceIdType.MESH,
        )
        copy.start()
        copies.append(copy)
    for copy in copies:
        copy.wait()


def gather_gains(gains, chan_count, sub_count):
    channels_here, _, directions, _ = gains.shape
    half = channels_here // sub_count
    return pl.pallas_call(
        functools.partial(gather_kernel, chan_count, sub_count, half),
        out_shape=jax.ShapeDtypeStruct(
            (chan_count, sub_count, 2, directions, LANES), jnp.float32
        ),
        in_specs=[pl.BlockSpec(memory_space=pltpu.VMEM)],
        out_specs=pl.BlockSpec(memory_space=pltpu.VMEM),
        scratch_shapes=[
            pltpu.VMEM((2, directions, LANES), jnp.float32),
            pltpu.SemaphoreType.DMA((chan_count,)),
            pltpu.SemaphoreType.DMA((chan_count,)),
        ],
        compiler_params=pltpu.CompilerParams(collective_id=1, has_side_effects=True),
    )(gains)


def solve_hermitian(groups_real, groups_imag, mixed, ridge, side_real, side_imag):
    directions = side_real.shape[0]
    middle = directions // 2
    row = lax.broadcasted_iota(jnp.int32, side_real.shape, 0)
    upper = row < middle
    swapped = pltpu.roll(mixed, middle, axis=0)
    real = {0: groups_real[0] + ridge, middle: jnp.where(upper, mixed, swapped)}
    imag = {0: jnp.zeros_like(ridge), middle: jnp.where(upper, -swapped, mixed)}
    for d in range(1, middle):
        real[d], imag[d] = groups_real[d], groups_imag[d - 1]
        real[directions - d] = pltpu.roll(groups_real[d], d, axis=0)
        imag[directions - d] = -pltpu.roll(groups_imag[d - 1], d, axis=0)
    columns = []
    for l in range(directions):
        column_real, column_imag = real[l], imag[l]
        for k in range(1, directions):
            here = row == k
            d = (l - k) % directions
            column_real = jnp.where(here, real[d], column_real)
            column_imag = jnp.where(here, imag[d], column_imag)
        columns.append((column_real, column_imag))
    columns.append((side_real, side_imag))
    scale = jnp.zeros_like(ridge)
    for j in range(directions):
        pivot_real, pivot_imag = columns[j]
        inverse = 1.0 / pivot_real[j : j + 1]
        here = row == j
        scale = jnp.where(here, jnp.broadcast_to(inverse, scale.shape), scale)
        factor_real = jnp.where(here, 0.0, pivot_real * inverse)
        factor_imag = jnp.where(here, 0.0, pivot_imag * inverse)
        for l in range(j + 1, directions + 1):
            value_real, value_imag = columns[l]
            head_real, head_imag = value_real[j : j + 1], value_imag[j : j + 1]
            columns[l] = (
                value_real - (factor_real * head_real - factor_imag * head_imag),
                value_imag - (factor_real * head_imag + factor_imag * head_real),
            )
    return columns[-1][0] * scale, columns[-1][1] * scale


def basis_of(channel, channels):
    x = (2.0 * channel - (channels - 1)) / max(channels - 1, 1)
    return [
        jnp.ones_like(x),
        x,
        0.5 * (3.0 * x * x - 1.0),
        0.5 * (5.0 * x * x * x - 3.0 * x),
    ]


def inverse_gram(channels):
    f = np.arange(channels, dtype=np.float64)
    x = (2.0 * f - (channels - 1)) / max(channels - 1, 1)
    basis = np.stack([np.ones_like(x), x, 0.5 * (3 * x * x - 1), 0.5 * (5 * x * x * x - 3 * x)])
    return np.linalg.inv(basis @ basis.T)


def finish_kernel(
    chan_count,
    sub_count,
    half,
    rho_ref,
    packed_ref,
    duals_ref,
    consensus_ref,
    gains_out,
    consensus_out,
    duals_out,
    pad,
    near_buf,
    send_buf,
    far_buf,
    weights,
    basis_buf,
    near_send,
    near_recv,
    far_send,
    far_recv,
    last_send,
    last_recv,
):
    chan, sub = lax.axis_index("chan"), lax.axis_index("sub")
    owners = chan_count * sub_count
    channels = owners * half
    width = LANES // half
    directions, stations = duals_ref.shape[2], duals_ref.shape[3]
    degree = consensus_ref.shape[0]
    me = chan * sub_count + sub

    def device(flat):
        return {"chan": lax.div(flat, sub_count), "sub": lax.rem(flat, sub_count)}

    barrier = pltpu.get_barrier_semaphore()
    for offset in range(1, owners):
        pl.semaphore_signal(
            barrier,
            inc=1,
            device_id=device(lax.rem(me + offset, owners)),
            device_id_type=pl.DeviceIdType.MESH,
        )
    pl.semaphore_wait(barrier, owners - 1)

    order = list(range(1, chan_count)) + [0]
    near = {}
    for offset in order:
        target = lax.rem(chan + offset, chan_count)
        for shift in range(1, sub_count):
            other = lax.rem(sub + shift, sub_count)
            copy = pltpu.make_async_remote_copy(
                src_ref=packed_ref.at[target, other],
                dst_ref=near_buf.at[shift - 1, offset],
                send_sem=near_send.at[shift - 1, offset],
                recv_sem=near_recv.at[shift - 1, offset],
                device_id={"sub": other},
                device_id_type=pl.DeviceIdType.MESH,
            )
            copy.start()
            near[offset, shift] = copy

    pad[...] = jnp.zeros_like(pad)
    shape = (directions, LANES)
    row = lax.broadcasted_iota(jnp.int32, shape, 0)
    rho = jnp.zeros(shape, jnp.float32)
    for k in range(directions):
        rho = jnp.where(row == k, rho_ref[k], rho)
    lane = lax.broadcasted_iota(jnp.int32, (owners, LANES), 1)
    owner = lax.broadcasted_iota(jnp.int32, (owners, LANES), 0)
    everyone = basis_of((owner * half + lax.div(lane, width)).astype(jnp.float32), channels)
    for d in range(degree):
        basis_buf[d] = everyone[d]
    mine = [jnp.broadcast_to(basis_buf[d, pl.ds(me, 1), :], shape) for d in range(degree)]
    duals = [
        lay_pair(lambda number: duals_ref[number, part], pad, half, width) for part in range(2)
    ]
    anchors = []
    for part in range(2):
        anchor = jnp.zeros(shape, jnp.float32)
        for d in range(degree):
            anchor = anchor + mine[d] * lay_pair(
                lambda number: consensus_ref[d, part], pad, half, width
            )
        anchors.append(anchor)

    far = []
    for offset in order:
        target = lax.rem(chan + offset, chan_count)
        total = packed_ref[target, sub]
        for shift in range(1, sub_count):
            near[offset, shift].wait_recv()
            total = total + near_buf[shift - 1, offset]
        if offset:
            send_buf[offset] = total
            copy = pltpu.make_async_remote_copy(
                src_ref=send_buf.at[offset],
                dst_ref=far_buf.at[offset],
                send_sem=far_send.at[offset],
                recv_sem=far_recv.at[offset],
                device_id={"chan": target},
                device_id_type=pl.DeviceIdType.MESH,
            )
            copy.start()
            far.append((offset, copy))
    for offset, copy in far:
        copy.wait_recv()
        total = total + far_buf[offset]

    middle = directions // 2
    group = [total[i * directions : (i + 1) * directions] for i in range(directions + 2)]
    solved = solve_hermitian(
        group[:middle],
        group[middle : directions - 1],
        group[directions - 1],
        rho,
        group[directions] - duals[0] + rho * anchors[0],
        group[directions + 1] - duals[1] + rho * anchors[1],
    )
    for part in range(2):
        weights[me, part] = solved[part] + duals[part] / rho

    last = []
    for offset in range(1, owners):
        copy = pltpu.make_async_remote_copy(
            src_ref=weights.at[me],
            dst_ref=weights.at[me],
            send_sem=last_send.at[offset],
            recv_sem=last_recv.at[offset],
            device_id=device(lax.rem(me + offset, owners)),
            device_id_type=pl.DeviceIdType.MESH,
        )
        copy.start()
        last.append(copy)

    def store(ref, part, value):
        for number in range(half):
            turned = pltpu.roll(value, LANES - number * width, axis=1) if number else value
            ref[number, part] = turned[:, :stations]

    for part in range(2):
        store(gains_out, part, solved[part])
    for copy in last:
        copy.wait_recv()
    inverse = inverse_gram(channels)
    for part in range(2):
        totals = []
        for d in range(degree):
            value = jnp.zeros(shape, jnp.float32)
            for number in range(owners):
                value = value + basis_buf[d, number : number + 1, :] * weights[number, part]
            folded = value
            for number in range(1, half):
                folded = folded + pltpu.roll(value, number * width, axis=1)
            totals.append(folded)
        fitted = jnp.zeros(shape, jnp.float32)
        for d in range(degree):
            value = sum(float(inverse[d, e]) * totals[e] for e in range(degree))
            consensus_out[d, part] = value[:, :stations]
            fitted = fitted + mine[d] * value
        store(duals_out, part, duals[part] + rho * (solved[part] - fitted))
    for copy in near.values():
        copy.wait_send()
    for _, copy in far:
        copy.wait_send()
    for copy in last:
        copy.wait_send()


def finish(rho, packed, duals, consensus, chan_count, sub_count):
    half, _, directions, stations = duals.shape
    _, _, rows, _ = packed.shape
    owners = chan_count * sub_count
    degree = consensus.shape[0]
    vmem = pl.BlockSpec(memory_space=pltpu.VMEM)
    dma = pltpu.SemaphoreType.DMA
    return pl.pallas_call(
        functools.partial(finish_kernel, chan_count, sub_count, half),
        out_shape=(
            jax.ShapeDtypeStruct(duals.shape, jnp.float32),
            jax.ShapeDtypeStruct(consensus.shape, jnp.float32),
            jax.ShapeDtypeStruct(duals.shape, jnp.float32),
        ),
        in_specs=[pl.BlockSpec(memory_space=pltpu.SMEM), vmem, vmem, vmem],
        out_specs=(vmem, vmem, vmem),
        scratch_shapes=[
            pltpu.VMEM((2, directions, LANES), jnp.float32),
            pltpu.VMEM((sub_count - 1, chan_count, rows, LANES), jnp.float32),
            pltpu.VMEM((chan_count, rows, LANES), jnp.float32),
            pltpu.VMEM((chan_count, rows, LANES), jnp.float32),
            pltpu.VMEM((owners, 2, directions, LANES), jnp.float32),
            pltpu.VMEM((degree, owners, LANES), jnp.float32),
            dma((sub_count - 1, chan_count)),
            dma((sub_count - 1, chan_count)),
            dma((chan_count,)),
            dma((chan_count,)),
            dma((owners,)),
            dma((owners,)),
        ],
        compiler_params=pltpu.CompilerParams(
            collective_id=2, has_side_effects=True, vmem_limit_bytes=60 << 20
        ),
    )(rho, packed, duals, consensus)


def body(
    predicted_sky_response,
    measured_correlation,
    keep_indicator,
    tile_owner,
    tile_channel,
    tile_base,
    pairs,
    gains,
    duals,
    consensus,
    rho,
):
    channels_here, _, _, directions = gains.shape
    chan_count = lax.axis_size("chan")
    sub_count = lax.axis_size("sub")
    half = channels_here // sub_count
    all_gains = gather_gains(jnp.swapaxes(gains, 2, 3), chan_count, sub_count)
    full_channel = tile_owner[:, 0] * channels_here + tile_channel
    packed = accumulate(
        predicted_sky_response,
        measured_correlation,
        keep_indicator,
        full_channel,
        tile_base,
        pairs,
        all_gains.reshape(-1, directions, LANES),
        half,
    )
    outputs = finish(
        rho,
        packed.reshape((chan_count, sub_count) + packed.shape[1:]),
        jnp.swapaxes(duals, 2, 3),
        jnp.swapaxes(consensus, 2, 3),
        chan_count,
        sub_count,
    )
    return tuple(jnp.swapaxes(x, 2, 3) for x in outputs)


def solution(mesh):
    placed = (
        P(("groups", "chan", "sub"), None, None, None),
        P(("groups", "chan", "sub"), None, None),
        P(("groups", "chan", "sub"), None),
        P(("groups", "chan", "sub"), None),
        P(("groups", "chan", "sub")),
        P(("groups", "chan", "sub")),
        P(),
        P(("groups", "chan"), None, None, None),
        P(("groups", "chan", "sub"), None, None, None),
        P("groups", None, None, None),
        P(),
    )
    return jax.shard_map(
        body,
        mesh=mesh,
        in_specs=placed,
        out_specs=(
            P(("groups", "chan", "sub"), None, None, None),
            P("groups", None, None, None),
            P(("groups", "chan", "sub"), None, None, None),
        ),
        check_vma=False,
    )
```

```python
import functools
import math

import jax
import jax.numpy as jnp
import numpy as np
from jax import lax
from jax.experimental import pallas as pl
from jax.experimental.pallas import tpu as pltpu
from jax.sharding import PartitionSpec as P

LANES = 128


def hermitian_rows(real, imag, upper):
    half = real.shape[0] // 2
    groups_real = [real * real + imag * imag]
    groups_imag = []
    for shift in range(1, half + 1):
        turned_real = pltpu.roll(real, 2 * half - shift, axis=0)
        turned_imag = pltpu.roll(imag, 2 * half - shift, axis=0)
        groups_real.append(real * turned_real + imag * turned_imag)
        groups_imag.append(real * turned_imag - imag * turned_real)
    mixed = jnp.where(upper, groups_real.pop(), groups_imag.pop())
    return groups_real + groups_imag + [mixed]


def accumulate_kernel(
    block,
    unroll,
    half,
    sub_count,
    owner_ref,
    channel_ref,
    base_ref,
    coupling_ref,
    observed_ref,
    keep_ref,
    pairs_ref,
    gains_ref,
    out_ref,
    table,
    turned,
    coupling_f,
    observed_f,
    keep_f,
):
    step = pl.program_id(0)
    bases = pairs_ref.shape[0]
    tile_rows = keep_ref.shape[1]
    width = LANES // half
    directions = gains_ref.shape[1]

    @pl.when(step == 0)
    def _():
        out_ref[...] = jnp.zeros_like(out_ref)
        turned[...] = jnp.zeros_like(turned)
        for base in range(bases):
            turned[2 * base : 2 * base + 2, :] = pairs_ref[base].astype(jnp.float32)
        columns = jnp.transpose(turned[...])
        lane = lax.broadcasted_iota(jnp.int32, (tile_rows, LANES), 1).astype(jnp.float32)
        for base in range(bases):
            for end in range(2):
                station = jnp.broadcast_to(
                    columns[:, 2 * base + end : 2 * base + end + 1], lane.shape
                )
                for part in range(half):
                    table[base * half + part, end * tile_rows : (end + 1) * tile_rows, :] = (
                        jnp.where(station == lane - float(part * width), 1.0, 0.0).astype(jnp.bfloat16)
                    )

    coupling_f[...] = coupling_ref[...].astype(jnp.float32)
    observed_f[...] = observed_ref[...].astype(jnp.float32)
    keep_f[...] = jnp.where(keep_ref[...] > 0, 1.0, 0.0)
    upper = lax.broadcasted_iota(jnp.int32, (directions, LANES), 0) < directions // 2

    def spread(row):
        return jnp.broadcast_to(row, (directions, LANES))

    def one_tile(local):
        tile = step * block + local
        channel = channel_ref[tile]
        base = base_ref[tile]
        owner = owner_ref[tile] * sub_count + lax.div(channel, half)
        place = lax.rem(channel, half)
        kept = spread(keep_f[pl.ds(local, 1), :])
        first = local * 2 * directions
        real = coupling_f[pl.ds(first, directions, stride=2), :] * kept
        imag = coupling_f[pl.ds(first + 1, directions, stride=2), :] * kept
        seen_real = spread(observed_f[pl.ds(2 * local, 1), :])
        seen_imag = spread(observed_f[pl.ds(2 * local + 1, 1), :])
        near = spread(pairs_ref[base, pl.ds(0, 1), :])
        far = spread(pairs_ref[base, pl.ds(1, 1), :])
        near, far = near + place * width, far + place * width
        gain_real = gains_ref[2 * owner]
        gain_imag = gains_ref[2 * owner + 1]

        def pick(values, index):
            return jnp.take_along_axis(values, index, axis=1, mode="promise_in_bounds")

        near_real, near_imag = pick(gain_real, near), pick(gain_imag, near)
        far_real, far_imag = pick(gain_real, far), pick(gain_imag, far)
        slope_real = real * far_real + imag * far_imag
        slope_imag = imag * far_real - real * far_imag
        mirror_real = real * near_real - imag * near_imag
        mirror_imag = -(real * near_imag + imag * near_real)

        def end_rows(vector_real, vector_imag, weight_real, weight_imag):
            side_real = vector_real * weight_real + vector_imag * weight_imag
            side_imag = vector_real * weight_imag - vector_imag * weight_real
            groups = hermitian_rows(vector_real, vector_imag, upper)
            whole = jnp.concatenate(groups, axis=0).astype(jnp.bfloat16)
            side = jnp.concatenate([side_real, side_imag], axis=0)
            high = side.astype(jnp.bfloat16)
            low = (side - high.astype(jnp.float32)).astype(jnp.bfloat16)
            return jnp.concatenate([whole, high, low], axis=0)

        rows = jnp.concatenate(
            [
                end_rows(slope_real, slope_imag, seen_real, seen_imag),
                end_rows(mirror_real, mirror_imag, seen_real, -seen_imag),
            ],
            axis=1,
        )
        sums = jnp.dot(rows, table[base * half + place], preferred_element_type=jnp.float32)
        normal_rows = directions * directions
        return owner, jnp.concatenate(
            [
                sums[:normal_rows],
                sums[normal_rows : normal_rows + 2 * directions] + sums[normal_rows + 2 * directions :],
            ],
            axis=0,
        )

    def one_group(group, carry):
        results = [one_tile(group * unroll + number) for number in range(unroll)]
        for owner, sums in results:
            out_ref[owner] += sums
        return carry

    lax.fori_loop(0, block // unroll, one_group, 0)


def accumulate(coupling, observed, keep, owner, channel, base, pairs, gain_table, half, sub_count):
    tiles, directions, _, tile_rows = coupling.shape
    owners = gain_table.shape[0] // 2
    bases = pairs.shape[0]
    block = min(64, tiles)
    unroll = math.gcd(block, 32)
    kernel = functools.partial(accumulate_kernel, block, unroll, half, sub_count)
    out_rows = directions * directions + 2 * directions
    return pl.pallas_call(
        kernel,
        grid_spec=pltpu.PrefetchScalarGridSpec(
            num_scalar_prefetch=3,
            grid=(tiles // block,),
            in_specs=[
                pl.BlockSpec((block * 2 * directions, tile_rows), lambda i, *_: (i, 0)),
                pl.BlockSpec((block * 2, tile_rows), lambda i, *_: (i, 0)),
                pl.BlockSpec((block, tile_rows), lambda i, *_: (i, 0)),
                pl.BlockSpec(pairs.shape, lambda i, *_: (0, 0, 0)),
                pl.BlockSpec(gain_table.shape, lambda i, *_: (0, 0, 0)),
            ],
            out_specs=pl.BlockSpec(
                (owners, out_rows, LANES), lambda i, *_: (0, 0, 0)
            ),
            scratch_shapes=[
                pltpu.VMEM((bases * half, 2 * tile_rows, LANES), jnp.bfloat16),
                pltpu.VMEM((LANES, tile_rows), jnp.float32),
                pltpu.VMEM((block * 2 * directions, tile_rows), jnp.float32),
                pltpu.VMEM((block * 2, tile_rows), jnp.float32),
                pltpu.VMEM((block, tile_rows), jnp.float32),
            ],
        ),
        out_shape=jax.ShapeDtypeStruct((owners, out_rows, LANES), jnp.float32),
        compiler_params=pltpu.CompilerParams(
            dimension_semantics=("arbitrary",), vmem_limit_bytes=60 << 20
        ),
    )(
        owner,
        channel,
        base,
        coupling.reshape(tiles * 2 * directions, tile_rows),
        observed.reshape(tiles * 2, tile_rows),
        keep,
        pairs,
        gain_table,
    )


def lay_pair(load, pad, half, width):
    total = None
    for part in range(half):
        block = load(part)
        pad[part % 2, :, : block.shape[1]] = block
        value = pad[part % 2]
        if part:
            value = pltpu.roll(value, part * width, axis=1)
        total = value if total is None else total + value
    return total


def gather_kernel(chan_count, sub_count, half, gains_ref, out_ref, pad, send_sem, recv_sem):
    chan = lax.axis_index("chan")
    width = LANES // half
    pad[...] = jnp.zeros_like(pad)
    for owner in range(sub_count):
        for part in range(2):
            out_ref[chan, owner, part] = lay_pair(
                lambda number: gains_ref[owner * half + number, part], pad, half, width
            )
    barrier = pltpu.get_barrier_semaphore()
    for offset in range(1, chan_count):
        pl.semaphore_signal(
            barrier,
            inc=1,
            device_id={"chan": lax.rem(chan + offset, chan_count)},
            device_id_type=pl.DeviceIdType.MESH,
        )
    pl.semaphore_wait(barrier, chan_count - 1)
    copies = []
    for offset in range(1, chan_count):
        copy = pltpu.make_async_remote_copy(
            src_ref=out_ref.at[chan],
            dst_ref=out_ref.at[chan],
            send_sem=send_sem.at[offset],
            recv_sem=recv_sem.at[offset],
            device_id={"chan": lax.rem(chan + offset, chan_count)},
            device_id_type=pl.DeviceIdType.MESH,
        )
        copy.start()
        copies.append(copy)
    for copy in copies:
        copy.wait()


def gather_gains(gains, chan_count, sub_count):
    channels_here, _, directions, _ = gains.shape
    half = channels_here // sub_count
    return pl.pallas_call(
        functools.partial(gather_kernel, chan_count, sub_count, half),
        out_shape=jax.ShapeDtypeStruct(
            (chan_count, sub_count, 2, directions, LANES), jnp.float32
        ),
        in_specs=[pl.BlockSpec(memory_space=pltpu.VMEM)],
        out_specs=pl.BlockSpec(memory_space=pltpu.VMEM),
        scratch_shapes=[
            pltpu.VMEM((2, directions, LANES), jnp.float32),
            pltpu.SemaphoreType.DMA((chan_count,)),
            pltpu.SemaphoreType.DMA((chan_count,)),
        ],
        compiler_params=pltpu.CompilerParams(collective_id=1, has_side_effects=True),
    )(gains)


def solve_hermitian(groups_real, groups_imag, mixed, ridge, side_real, side_imag):
    directions = side_real.shape[0]
    middle = directions // 2
    row = lax.broadcasted_iota(jnp.int32, side_real.shape, 0)
    upper = row < middle
    swapped = pltpu.roll(mixed, middle, axis=0)
    real = {0: groups_real[0] + ridge, middle: jnp.where(upper, mixed, swapped)}
    imag = {0: jnp.zeros_like(ridge), middle: jnp.where(upper, -swapped, mixed)}
    for d in range(1, middle):
        real[d], imag[d] = groups_real[d], groups_imag[d - 1]
        real[directions - d] = pltpu.roll(groups_real[d], d, axis=0)
        imag[directions - d] = -pltpu.roll(groups_imag[d - 1], d, axis=0)
    columns = []
    for l in range(directions):
        column_real, column_imag = real[l], imag[l]
        for k in range(1, directions):
            here = row == k
            d = (l - k) % directions
            column_real = jnp.where(here, real[d], column_real)
            column_imag = jnp.where(here, imag[d], column_imag)
        columns.append((column_real, column_imag))
    columns.append((side_real, side_imag))
    scale = jnp.zeros_like(ridge)
    for j in range(directions):
        pivot_real, pivot_imag = columns[j]
        inverse = 1.0 / pivot_real[j : j + 1]
        here = row == j
        scale = jnp.where(here, jnp.broadcast_to(inverse, scale.shape), scale)
        factor_real = jnp.where(here, 0.0, pivot_real * inverse)
        factor_imag = jnp.where(here, 0.0, pivot_imag * inverse)
        for l in range(j + 1, directions + 1):
            value_real, value_imag = columns[l]
            head_real, head_imag = value_real[j : j + 1], value_imag[j : j + 1]
            columns[l] = (
                value_real - (factor_real * head_real - factor_imag * head_imag),
                value_imag - (factor_real * head_imag + factor_imag * head_real),
            )
    return columns[-1][0] * scale, columns[-1][1] * scale


def basis_of(channel, channels):
    x = (2.0 * channel - (channels - 1)) / max(channels - 1, 1)
    return [
        jnp.ones_like(x),
        x,
        0.5 * (3.0 * x * x - 1.0),
        0.5 * (5.0 * x * x * x - 3.0 * x),
    ]


def inverse_gram(channels):
    f = np.arange(channels, dtype=np.float64)
    x = (2.0 * f - (channels - 1)) / max(channels - 1, 1)
    basis = np.stack([np.ones_like(x), x, 0.5 * (3 * x * x - 1), 0.5 * (5 * x * x * x - 3 * x)])
    return np.linalg.inv(basis @ basis.T)


def encode(sums, directions):
    normal_rows = directions * directions
    side = sums[normal_rows:]
    high = side.astype(jnp.bfloat16)
    low = (side - high.astype(jnp.float32)).astype(jnp.bfloat16)
    return jnp.concatenate([sums[:normal_rows].astype(jnp.bfloat16), high, low], axis=0)


def decode(coded, directions):
    wide = coded.astype(jnp.float32)
    normal_rows = directions * directions
    side_rows = 2 * directions
    high, low = wide[normal_rows : normal_rows + side_rows], wide[normal_rows + side_rows :]
    return jnp.concatenate([wide[:normal_rows], high + low], axis=0)


def finish_kernel(
    chan_count,
    sub_count,
    half,
    rho_ref,
    packed_ref,
    duals_ref,
    consensus_ref,
    gains_out,
    consensus_out,
    duals_out,
    pad,
    near_src,
    near_buf,
    send_buf,
    far_buf,
    weights,
    basis_buf,
    near_send,
    near_recv,
    far_send,
    far_recv,
    last_send,
    last_recv,
):
    chan, sub = lax.axis_index("chan"), lax.axis_index("sub")
    owners = chan_count * sub_count
    channels = owners * half
    width = LANES // half
    directions, stations = duals_ref.shape[2], duals_ref.shape[3]
    degree = consensus_ref.shape[0]
    me = chan * sub_count + sub

    def device(flat):
        return {"chan": lax.div(flat, sub_count), "sub": lax.rem(flat, sub_count)}

    barrier = pltpu.get_barrier_semaphore()
    for offset in range(1, owners):
        pl.semaphore_signal(
            barrier,
            inc=1,
            device_id=device(lax.rem(me + offset, owners)),
            device_id_type=pl.DeviceIdType.MESH,
        )
    order = list(range(1, chan_count)) + [0]
    for offset in order:
        target = lax.rem(chan + offset, chan_count)
        for shift in range(1, sub_count):
            near_src[shift - 1, offset] = encode(
                packed_ref[target, lax.rem(sub + shift, sub_count)], directions
            )
    pl.semaphore_wait(barrier, owners - 1)

    near = {}
    for offset in order:
        for shift in range(1, sub_count):
            other = lax.rem(sub + shift, sub_count)
            copy = pltpu.make_async_remote_copy(
                src_ref=near_src.at[shift - 1, offset],
                dst_ref=near_buf.at[shift - 1, offset],
                send_sem=near_send.at[shift - 1, offset],
                recv_sem=near_recv.at[shift - 1, offset],
                device_id={"sub": other},
                device_id_type=pl.DeviceIdType.MESH,
            )
            copy.start()
            near[offset, shift] = copy

    pad[...] = jnp.zeros_like(pad)
    shape = (directions, LANES)
    row = lax.broadcasted_iota(jnp.int32, shape, 0)
    rho = jnp.zeros(shape, jnp.float32)
    for k in range(directions):
        rho = jnp.where(row == k, rho_ref[k], rho)
    lane = lax.broadcasted_iota(jnp.int32, (owners, LANES), 1)
    owner = lax.broadcasted_iota(jnp.int32, (owners, LANES), 0)
    everyone = basis_of((owner * half + lax.div(lane, width)).astype(jnp.float32), channels)
    for d in range(degree):
        basis_buf[d] = everyone[d]
    mine = [jnp.broadcast_to(basis_buf[d, pl.ds(me, 1), :], shape) for d in range(degree)]
    duals = [
        lay_pair(lambda number: duals_ref[number, part], pad, half, width) for part in range(2)
    ]
    anchors = []
    for part in range(2):
        anchor = jnp.zeros(shape, jnp.float32)
        for d in range(degree):
            anchor = anchor + mine[d] * lay_pair(
                lambda number: consensus_ref[d, part], pad, half, width
            )
        anchors.append(anchor)

    far = []
    for offset in order:
        target = lax.rem(chan + offset, chan_count)
        total = packed_ref[target, sub]
        for shift in range(1, sub_count):
            near[offset, shift].wait_recv()
            total = total + decode(near_buf[shift - 1, offset], directions)
        if offset:
            send_buf[offset] = encode(total, directions)
            copy = pltpu.make_async_remote_copy(
                src_ref=send_buf.at[offset],
                dst_ref=far_buf.at[offset],
                send_sem=far_send.at[offset],
                recv_sem=far_recv.at[offset],
                device_id={"chan": target},
                device_id_type=pl.DeviceIdType.MESH,
            )
            copy.start()
            far.append((offset, copy))
    for offset, copy in far:
        copy.wait_recv()
        total = total + decode(far_buf[offset], directions)

    middle = directions // 2
    group = [total[i * directions : (i + 1) * directions] for i in range(directions + 2)]
    solved = solve_hermitian(
        group[:middle],
        group[middle : directions - 1],
        group[directions - 1],
        rho,
        group[directions] - duals[0] + rho * anchors[0],
        group[directions + 1] - duals[1] + rho * anchors[1],
    )
    for part in range(2):
        weights[me, part] = solved[part] + duals[part] / rho

    last = []
    for offset in range(1, owners):
        copy = pltpu.make_async_remote_copy(
            src_ref=weights.at[me],
            dst_ref=weights.at[me],
            send_sem=last_send.at[offset],
            recv_sem=last_recv.at[offset],
            device_id=device(lax.rem(me + offset, owners)),
            device_id_type=pl.DeviceIdType.MESH,
        )
        copy.start()
        last.append(copy)

    def store(ref, part, value):
        for number in range(half):
            turned = pltpu.roll(value, LANES - number * width, axis=1) if number else value
            ref[number, part] = turned[:, :stations]

    for part in range(2):
        store(gains_out, part, solved[part])
    for copy in last:
        copy.wait_recv()
    inverse = inverse_gram(channels)
    for part in range(2):
        totals = []
        for d in range(degree):
            value = jnp.zeros(shape, jnp.float32)
            for number in range(owners):
                value = value + basis_buf[d, number : number + 1, :] * weights[number, part]
            folded = value
            for number in range(1, half):
                folded = folded + pltpu.roll(value, number * width, axis=1)
            totals.append(folded)
        fitted = jnp.zeros(shape, jnp.float32)
        for d in range(degree):
            value = sum(float(inverse[d, e]) * totals[e] for e in range(degree))
            consensus_out[d, part] = value[:, :stations]
            fitted = fitted + mine[d] * value
        store(duals_out, part, duals[part] + rho * (solved[part] - fitted))
    for copy in near.values():
        copy.wait_send()
    for _, copy in far:
        copy.wait_send()
    for copy in last:
        copy.wait_send()


def finish(rho, packed, duals, consensus, chan_count, sub_count):
    half, _, directions, stations = duals.shape
    _, _, rows, _ = packed.shape
    owners = chan_count * sub_count
    degree = consensus.shape[0]
    coded = rows + 2 * directions
    vmem = pl.BlockSpec(memory_space=pltpu.VMEM)
    dma = pltpu.SemaphoreType.DMA
    return pl.pallas_call(
        functools.partial(finish_kernel, chan_count, sub_count, half),
        out_shape=(
            jax.ShapeDtypeStruct(duals.shape, jnp.float32),
            jax.ShapeDtypeStruct(consensus.shape, jnp.float32),
            jax.ShapeDtypeStruct(duals.shape, jnp.float32),
        ),
        in_specs=[pl.BlockSpec(memory_space=pltpu.SMEM), vmem, vmem, vmem],
        out_specs=(vmem, vmem, vmem),
        scratch_shapes=[
            pltpu.VMEM((2, directions, LANES), jnp.float32),
            pltpu.VMEM((sub_count - 1, chan_count, coded, LANES), jnp.bfloat16),
            pltpu.VMEM((sub_count - 1, chan_count, coded, LANES), jnp.bfloat16),
            pltpu.VMEM((chan_count, coded, LANES), jnp.bfloat16),
            pltpu.VMEM((chan_count, coded, LANES), jnp.bfloat16),
            pltpu.VMEM((owners, 2, directions, LANES), jnp.float32),
            pltpu.VMEM((degree, owners, LANES), jnp.float32),
            dma((sub_count - 1, chan_count)),
            dma((sub_count - 1, chan_count)),
            dma((chan_count,)),
            dma((chan_count,)),
            dma((owners,)),
            dma((owners,)),
        ],
        compiler_params=pltpu.CompilerParams(
            collective_id=2, has_side_effects=True, vmem_limit_bytes=60 << 20
        ),
    )(rho, packed, duals, consensus)


def body(
    predicted_sky_response,
    measured_correlation,
    keep_indicator,
    tile_owner,
    tile_channel,
    tile_base,
    pairs,
    gains,
    duals,
    consensus,
    rho,
):
    channels_here, _, _, directions = gains.shape
    chan_count = lax.axis_size("chan")
    sub_count = lax.axis_size("sub")
    half = channels_here // sub_count
    all_gains = gather_gains(jnp.swapaxes(gains, 2, 3), chan_count, sub_count)
    packed = accumulate(
        predicted_sky_response,
        measured_correlation,
        keep_indicator,
        tile_owner[:, 0],
        tile_channel,
        tile_base,
        pairs,
        all_gains.reshape(-1, directions, LANES),
        half,
        sub_count,
    )
    outputs = finish(
        rho,
        packed.reshape((chan_count, sub_count) + packed.shape[1:]),
        jnp.swapaxes(duals, 2, 3),
        jnp.swapaxes(consensus, 2, 3),
        chan_count,
        sub_count,
    )
    return tuple(jnp.swapaxes(x, 2, 3) for x in outputs)


def solution(mesh):
    placed = (
        P(("groups", "chan", "sub"), None, None, None),
        P(("groups", "chan", "sub"), None, None),
        P(("groups", "chan", "sub"), None),
        P(("groups", "chan", "sub"), None),
        P(("groups", "chan", "sub")),
        P(("groups", "chan", "sub")),
        P(),
        P(("groups", "chan"), None, None, None),
        P(("groups", "chan", "sub"), None, None, None),
        P("groups", None, None, None),
        P(),
    )
    return jax.shard_map(
        body,
        mesh=mesh,
        in_specs=placed,
        out_specs=(
            P(("groups", "chan", "sub"), None, None, None),
            P("groups", None, None, None),
            P(("groups", "chan", "sub"), None, None, None),
        ),
        check_vma=False,
    )
```

```python
import functools
import math

import jax
import jax.numpy as jnp
import numpy as np
from jax import lax
from jax.experimental import pallas as pl
from jax.experimental.pallas import tpu as pltpu
from jax.sharding import PartitionSpec as P

LANES = 128


def hermitian_rows(real, imag, upper):
    half = real.shape[0] // 2
    groups_real = [real * real + imag * imag]
    groups_imag = []
    for shift in range(1, half + 1):
        turned_real = pltpu.roll(real, 2 * half - shift, axis=0)
        turned_imag = pltpu.roll(imag, 2 * half - shift, axis=0)
        groups_real.append(real * turned_real + imag * turned_imag)
        groups_imag.append(real * turned_imag - imag * turned_real)
    mixed = jnp.where(upper, groups_real.pop(), groups_imag.pop())
    return groups_real + groups_imag + [mixed]


def accumulate_kernel(
    block,
    unroll,
    half,
    sub_count,
    owner_ref,
    channel_ref,
    base_ref,
    coupling_ref,
    observed_ref,
    keep_ref,
    pairs_ref,
    gains_ref,
    out_ref,
    table,
    turned,
    coupling_f,
    observed_f,
    keep_f,
):
    step = pl.program_id(0)
    bases = pairs_ref.shape[0]
    tile_rows = keep_ref.shape[1]
    width = LANES // half
    directions = gains_ref.shape[1]

    @pl.when(step == 0)
    def _():
        out_ref[...] = jnp.zeros_like(out_ref)
        turned[...] = jnp.zeros_like(turned)
        for base in range(bases):
            turned[2 * base : 2 * base + 2, :] = pairs_ref[base].astype(jnp.float32)
        columns = jnp.transpose(turned[...])
        lane = lax.broadcasted_iota(jnp.int32, (tile_rows, LANES), 1).astype(jnp.float32)
        for base in range(bases):
            for end in range(2):
                station = jnp.broadcast_to(
                    columns[:, 2 * base + end : 2 * base + end + 1], lane.shape
                )
                for part in range(half):
                    table[base * half + part, end * tile_rows : (end + 1) * tile_rows, :] = (
                        jnp.where(station == lane - float(part * width), 1.0, 0.0).astype(jnp.bfloat16)
                    )

    coupling_f[...] = coupling_ref[...].astype(jnp.float32)
    observed_f[...] = observed_ref[...].astype(jnp.float32)
    keep_f[...] = jnp.where(keep_ref[...] > 0, 1.0, 0.0)
    upper = lax.broadcasted_iota(jnp.int32, (directions, LANES), 0) < directions // 2

    def spread(row):
        return jnp.broadcast_to(row, (directions, LANES))

    def one_tile(local):
        tile = step * block + local
        channel = channel_ref[tile]
        base = base_ref[tile]
        owner = owner_ref[tile] * sub_count + lax.div(channel, half)
        place = lax.rem(channel, half)
        kept = spread(keep_f[pl.ds(local, 1), :])
        first = local * 2 * directions
        real = coupling_f[pl.ds(first, directions, stride=2), :] * kept
        imag = coupling_f[pl.ds(first + 1, directions, stride=2), :] * kept
        seen_real = spread(observed_f[pl.ds(2 * local, 1), :])
        seen_imag = spread(observed_f[pl.ds(2 * local + 1, 1), :])
        near = spread(pairs_ref[base, pl.ds(0, 1), :])
        far = spread(pairs_ref[base, pl.ds(1, 1), :])
        near, far = near + place * width, far + place * width
        gain_real = gains_ref[2 * owner]
        gain_imag = gains_ref[2 * owner + 1]

        def pick(values, index):
            return jnp.take_along_axis(values, index, axis=1, mode="promise_in_bounds")

        near_real, near_imag = pick(gain_real, near), pick(gain_imag, near)
        far_real, far_imag = pick(gain_real, far), pick(gain_imag, far)
        slope_real = real * far_real + imag * far_imag
        slope_imag = imag * far_real - real * far_imag
        mirror_real = real * near_real - imag * near_imag
        mirror_imag = -(real * near_imag + imag * near_real)

        def end_rows(vector_real, vector_imag, weight_real, weight_imag):
            side_real = vector_real * weight_real + vector_imag * weight_imag
            side_imag = vector_real * weight_imag - vector_imag * weight_real
            groups = hermitian_rows(vector_real, vector_imag, upper)
            whole = jnp.concatenate(groups, axis=0).astype(jnp.bfloat16)
            side = jnp.concatenate([side_real, side_imag], axis=0)
            high = side.astype(jnp.bfloat16)
            low = (side - high.astype(jnp.float32)).astype(jnp.bfloat16)
            return jnp.concatenate([whole, high, low], axis=0)

        rows = jnp.concatenate(
            [
                end_rows(slope_real, slope_imag, seen_real, seen_imag),
                end_rows(mirror_real, mirror_imag, seen_real, -seen_imag),
            ],
            axis=1,
        )
        sums = jnp.dot(rows, table[base * half + place], preferred_element_type=jnp.float32)
        normal_rows = directions * directions
        return owner, jnp.concatenate(
            [
                sums[:normal_rows],
                sums[normal_rows : normal_rows + 2 * directions] + sums[normal_rows + 2 * directions :],
            ],
            axis=0,
        )

    def one_group(group, carry):
        results = [one_tile(group * unroll + number) for number in range(unroll)]
        for owner, sums in results:
            out_ref[owner] += sums
        return carry

    lax.fori_loop(0, block // unroll, one_group, 0)


def accumulate(coupling, observed, keep, owner, channel, base, pairs, gain_table, half, sub_count):
    tiles, directions, _, tile_rows = coupling.shape
    owners = gain_table.shape[0] // 2
    bases = pairs.shape[0]
    block = min(64, tiles)
    unroll = math.gcd(block, 64)
    kernel = functools.partial(accumulate_kernel, block, unroll, half, sub_count)
    out_rows = directions * directions + 2 * directions
    return pl.pallas_call(
        kernel,
        grid_spec=pltpu.PrefetchScalarGridSpec(
            num_scalar_prefetch=3,
            grid=(tiles // block,),
            in_specs=[
                pl.BlockSpec((block * 2 * directions, tile_rows), lambda i, *_: (i, 0)),
                pl.BlockSpec((block * 2, tile_rows), lambda i, *_: (i, 0)),
                pl.BlockSpec((block, tile_rows), lambda i, *_: (i, 0)),
                pl.BlockSpec(pairs.shape, lambda i, *_: (0, 0, 0)),
                pl.BlockSpec(gain_table.shape, lambda i, *_: (0, 0, 0)),
            ],
            out_specs=pl.BlockSpec(
                (owners, out_rows, LANES), lambda i, *_: (0, 0, 0)
            ),
            scratch_shapes=[
                pltpu.VMEM((bases * half, 2 * tile_rows, LANES), jnp.bfloat16),
                pltpu.VMEM((LANES, tile_rows), jnp.float32),
                pltpu.VMEM((block * 2 * directions, tile_rows), jnp.float32),
                pltpu.VMEM((block * 2, tile_rows), jnp.float32),
                pltpu.VMEM((block, tile_rows), jnp.float32),
            ],
        ),
        out_shape=jax.ShapeDtypeStruct((owners, out_rows, LANES), jnp.float32),
        compiler_params=pltpu.CompilerParams(
            dimension_semantics=("arbitrary",), vmem_limit_bytes=60 << 20
        ),
    )(
        owner,
        channel,
        base,
        coupling.reshape(tiles * 2 * directions, tile_rows),
        observed.reshape(tiles * 2, tile_rows),
        keep,
        pairs,
        gain_table,
    )


def lay_pair(load, pad, half, width):
    total = None
    for part in range(half):
        block = load(part)
        pad[part % 2, :, : block.shape[1]] = block
        value = pad[part % 2]
        if part:
            value = pltpu.roll(value, part * width, axis=1)
        total = value if total is None else total + value
    return total


def gather_kernel(chan_count, sub_count, half, gains_ref, out_ref, pad, send_sem, recv_sem):
    chan = lax.axis_index("chan")
    width = LANES // half
    pad[...] = jnp.zeros_like(pad)
    for owner in range(sub_count):
        for part in range(2):
            out_ref[chan, owner, part] = lay_pair(
                lambda number: gains_ref[owner * half + number, part], pad, half, width
            )
    barrier = pltpu.get_barrier_semaphore()
    for offset in range(1, chan_count):
        pl.semaphore_signal(
            barrier,
            inc=1,
            device_id={"chan": lax.rem(chan + offset, chan_count)},
            device_id_type=pl.DeviceIdType.MESH,
        )
    pl.semaphore_wait(barrier, chan_count - 1)
    copies = []
    for offset in range(1, chan_count):
        copy = pltpu.make_async_remote_copy(
            src_ref=out_ref.at[chan],
            dst_ref=out_ref.at[chan],
            send_sem=send_sem.at[offset],
            recv_sem=recv_sem.at[offset],
            device_id={"chan": lax.rem(chan + offset, chan_count)},
            device_id_type=pl.DeviceIdType.MESH,
        )
        copy.start()
        copies.append(copy)
    for copy in copies:
        copy.wait()


def gather_gains(gains, chan_count, sub_count):
    channels_here, _, directions, _ = gains.shape
    half = channels_here // sub_count
    return pl.pallas_call(
        functools.partial(gather_kernel, chan_count, sub_count, half),
        out_shape=jax.ShapeDtypeStruct(
            (chan_count, sub_count, 2, directions, LANES), jnp.float32
        ),
        in_specs=[pl.BlockSpec(memory_space=pltpu.VMEM)],
        out_specs=pl.BlockSpec(memory_space=pltpu.VMEM),
        scratch_shapes=[
            pltpu.VMEM((2, directions, LANES), jnp.float32),
            pltpu.SemaphoreType.DMA((chan_count,)),
            pltpu.SemaphoreType.DMA((chan_count,)),
        ],
        compiler_params=pltpu.CompilerParams(collective_id=1, has_side_effects=True),
    )(gains)


def solve_hermitian(groups_real, groups_imag, mixed, ridge, side_real, side_imag):
    directions = side_real.shape[0]
    middle = directions // 2
    row = lax.broadcasted_iota(jnp.int32, side_real.shape, 0)
    upper = row < middle
    swapped = pltpu.roll(mixed, middle, axis=0)
    real = {0: groups_real[0] + ridge, middle: jnp.where(upper, mixed, swapped)}
    imag = {0: jnp.zeros_like(ridge), middle: jnp.where(upper, -swapped, mixed)}
    for d in range(1, middle):
        real[d], imag[d] = groups_real[d], groups_imag[d - 1]
        real[directions - d] = pltpu.roll(groups_real[d], d, axis=0)
        imag[directions - d] = -pltpu.roll(groups_imag[d - 1], d, axis=0)
    columns = []
    for l in range(directions):
        column_real, column_imag = real[l], imag[l]
        for k in range(1, directions):
            here = row == k
            d = (l - k) % directions
            column_real = jnp.where(here, real[d], column_real)
            column_imag = jnp.where(here, imag[d], column_imag)
        columns.append((column_real, column_imag))
    columns.append((side_real, side_imag))
    scale = jnp.zeros_like(ridge)
    for j in range(directions):
        pivot_real, pivot_imag = columns[j]
        inverse = 1.0 / pivot_real[j : j + 1]
        here = row == j
        scale = jnp.where(here, jnp.broadcast_to(inverse, scale.shape), scale)
        factor_real = jnp.where(here, 0.0, pivot_real * inverse)
        factor_imag = jnp.where(here, 0.0, pivot_imag * inverse)
        for l in range(j + 1, directions + 1):
            value_real, value_imag = columns[l]
            head_real, head_imag = value_real[j : j + 1], value_imag[j : j + 1]
            columns[l] = (
                value_real - (factor_real * head_real - factor_imag * head_imag),
                value_imag - (factor_real * head_imag + factor_imag * head_real),
            )
    return columns[-1][0] * scale, columns[-1][1] * scale


def basis_of(channel, channels):
    x = (2.0 * channel - (channels - 1)) / max(channels - 1, 1)
    return [
        jnp.ones_like(x),
        x,
        0.5 * (3.0 * x * x - 1.0),
        0.5 * (5.0 * x * x * x - 3.0 * x),
    ]


def inverse_gram(channels):
    f = np.arange(channels, dtype=np.float64)
    x = (2.0 * f - (channels - 1)) / max(channels - 1, 1)
    basis = np.stack([np.ones_like(x), x, 0.5 * (3 * x * x - 1), 0.5 * (5 * x * x * x - 3 * x)])
    return np.linalg.inv(basis @ basis.T)


def encode(sums, directions):
    normal_rows = directions * directions
    side = sums[normal_rows:]
    high = side.astype(jnp.bfloat16)
    low = (side - high.astype(jnp.float32)).astype(jnp.bfloat16)
    return jnp.concatenate([sums[:normal_rows].astype(jnp.bfloat16), high, low], axis=0)


def decode(coded, directions):
    wide = coded.astype(jnp.float32)
    normal_rows = directions * directions
    side_rows = 2 * directions
    high, low = wide[normal_rows : normal_rows + side_rows], wide[normal_rows + side_rows :]
    return jnp.concatenate([wide[:normal_rows], high + low], axis=0)


def finish_kernel(
    chan_count,
    sub_count,
    half,
    rho_ref,
    packed_ref,
    duals_ref,
    consensus_ref,
    gains_out,
    consensus_out,
    duals_out,
    pad,
    near_src,
    near_buf,
    send_buf,
    far_buf,
    weights,
    basis_buf,
    near_send,
    near_recv,
    far_send,
    far_recv,
    last_send,
    last_recv,
):
    chan, sub = lax.axis_index("chan"), lax.axis_index("sub")
    owners = chan_count * sub_count
    channels = owners * half
    width = LANES // half
    directions, stations = duals_ref.shape[2], duals_ref.shape[3]
    degree = consensus_ref.shape[0]
    me = chan * sub_count + sub

    def device(flat):
        return {"chan": lax.div(flat, sub_count), "sub": lax.rem(flat, sub_count)}

    barrier = pltpu.get_barrier_semaphore()
    for offset in range(1, owners):
        pl.semaphore_signal(
            barrier,
            inc=1,
            device_id=device(lax.rem(me + offset, owners)),
            device_id_type=pl.DeviceIdType.MESH,
        )
    order = list(range(1, chan_count)) + [0]
    for offset in order:
        target = lax.rem(chan + offset, chan_count)
        for shift in range(1, sub_count):
            near_src[shift - 1, offset] = encode(
                packed_ref[target, lax.rem(sub + shift, sub_count)], directions
            )
    pl.semaphore_wait(barrier, owners - 1)

    near = {}
    for offset in order:
        for shift in range(1, sub_count):
            other = lax.rem(sub + shift, sub_count)
            copy = pltpu.make_async_remote_copy(
                src_ref=near_src.at[shift - 1, offset],
                dst_ref=near_buf.at[shift - 1, offset],
                send_sem=near_send.at[shift - 1, offset],
                recv_sem=near_recv.at[shift - 1, offset],
                device_id={"sub": other},
                device_id_type=pl.DeviceIdType.MESH,
            )
            copy.start()
            near[offset, shift] = copy

    pad[...] = jnp.zeros_like(pad)
    shape = (directions, LANES)
    row = lax.broadcasted_iota(jnp.int32, shape, 0)
    rho = jnp.zeros(shape, jnp.float32)
    for k in range(directions):
        rho = jnp.where(row == k, rho_ref[k], rho)
    lane = lax.broadcasted_iota(jnp.int32, (owners, LANES), 1)
    owner = lax.broadcasted_iota(jnp.int32, (owners, LANES), 0)
    everyone = basis_of((owner * half + lax.div(lane, width)).astype(jnp.float32), channels)
    for d in range(degree):
        basis_buf[d] = everyone[d]
    mine = [jnp.broadcast_to(basis_buf[d, pl.ds(me, 1), :], shape) for d in range(degree)]
    duals = [
        lay_pair(lambda number: duals_ref[number, part], pad, half, width) for part in range(2)
    ]
    anchors = []
    for part in range(2):
        anchor = jnp.zeros(shape, jnp.float32)
        for d in range(degree):
            anchor = anchor + mine[d] * lay_pair(
                lambda number: consensus_ref[d, part], pad, half, width
            )
        anchors.append(anchor)

    far = []
    for offset in order:
        target = lax.rem(chan + offset, chan_count)
        total = packed_ref[target, sub]
        for shift in range(1, sub_count):
            near[offset, shift].wait_recv()
            total = total + decode(near_buf[shift - 1, offset], directions)
        if offset:
            send_buf[offset] = encode(total, directions)
            copy = pltpu.make_async_remote_copy(
                src_ref=send_buf.at[offset],
                dst_ref=far_buf.at[offset],
                send_sem=far_send.at[offset],
                recv_sem=far_recv.at[offset],
                device_id={"chan": target},
                device_id_type=pl.DeviceIdType.MESH,
            )
            copy.start()
            far.append((offset, copy))
    for offset, copy in far:
        copy.wait_recv()
        total = total + decode(far_buf[offset], directions)

    middle = directions // 2
    group = [total[i * directions : (i + 1) * directions] for i in range(directions + 2)]
    solved = solve_hermitian(
        group[:middle],
        group[middle : directions - 1],
        group[directions - 1],
        rho,
        group[directions] - duals[0] + rho * anchors[0],
        group[directions + 1] - duals[1] + rho * anchors[1],
    )
    for part in range(2):
        weights[me, part] = solved[part] + duals[part] / rho

    last = []
    for offset in range(1, owners):
        copy = pltpu.make_async_remote_copy(
            src_ref=weights.at[me],
            dst_ref=weights.at[me],
            send_sem=last_send.at[offset],
            recv_sem=last_recv.at[offset],
            device_id=device(lax.rem(me + offset, owners)),
            device_id_type=pl.DeviceIdType.MESH,
        )
        copy.start()
        last.append(copy)

    def store(ref, part, value):
        for number in range(half):
            turned = pltpu.roll(value, LANES - number * width, axis=1) if number else value
            ref[number, part] = turned[:, :stations]

    for part in range(2):
        store(gains_out, part, solved[part])
    for copy in last:
        copy.wait_recv()
    inverse = inverse_gram(channels)
    for part in range(2):
        totals = []
        for d in range(degree):
            value = jnp.zeros(shape, jnp.float32)
            for number in range(owners):
                value = value + basis_buf[d, number : number + 1, :] * weights[number, part]
            folded = value
            for number in range(1, half):
                folded = folded + pltpu.roll(value, number * width, axis=1)
            totals.append(folded)
        fitted = jnp.zeros(shape, jnp.float32)
        for d in range(degree):
            value = sum(float(inverse[d, e]) * totals[e] for e in range(degree))
            consensus_out[d, part] = value[:, :stations]
            fitted = fitted + mine[d] * value
        store(duals_out, part, duals[part] + rho * (solved[part] - fitted))
    for copy in near.values():
        copy.wait_send()
    for _, copy in far:
        copy.wait_send()
    for copy in last:
        copy.wait_send()


def finish(rho, packed, duals, consensus, chan_count, sub_count):
    half, _, directions, stations = duals.shape
    _, _, rows, _ = packed.shape
    owners = chan_count * sub_count
    degree = consensus.shape[0]
    coded = rows + 2 * directions
    vmem = pl.BlockSpec(memory_space=pltpu.VMEM)
    dma = pltpu.SemaphoreType.DMA
    return pl.pallas_call(
        functools.partial(finish_kernel, chan_count, sub_count, half),
        out_shape=(
            jax.ShapeDtypeStruct(duals.shape, jnp.float32),
            jax.ShapeDtypeStruct(consensus.shape, jnp.float32),
            jax.ShapeDtypeStruct(duals.shape, jnp.float32),
        ),
        in_specs=[pl.BlockSpec(memory_space=pltpu.SMEM), vmem, vmem, vmem],
        out_specs=(vmem, vmem, vmem),
        scratch_shapes=[
            pltpu.VMEM((2, directions, LANES), jnp.float32),
            pltpu.VMEM((sub_count - 1, chan_count, coded, LANES), jnp.bfloat16),
            pltpu.VMEM((sub_count - 1, chan_count, coded, LANES), jnp.bfloat16),
            pltpu.VMEM((chan_count, coded, LANES), jnp.bfloat16),
            pltpu.VMEM((chan_count, coded, LANES), jnp.bfloat16),
            pltpu.VMEM((owners, 2, directions, LANES), jnp.float32),
            pltpu.VMEM((degree, owners, LANES), jnp.float32),
            dma((sub_count - 1, chan_count)),
            dma((sub_count - 1, chan_count)),
            dma((chan_count,)),
            dma((chan_count,)),
            dma((owners,)),
            dma((owners,)),
        ],
        compiler_params=pltpu.CompilerParams(
            collective_id=2, has_side_effects=True, vmem_limit_bytes=60 << 20
        ),
    )(rho, packed, duals, consensus)


def body(
    predicted_sky_response,
    measured_correlation,
    keep_indicator,
    tile_owner,
    tile_channel,
    tile_base,
    pairs,
    gains,
    duals,
    consensus,
    rho,
):
    channels_here, _, _, directions = gains.shape
    chan_count = lax.axis_size("chan")
    sub_count = lax.axis_size("sub")
    half = channels_here // sub_count
    all_gains = gather_gains(jnp.swapaxes(gains, 2, 3), chan_count, sub_count)
    packed = accumulate(
        predicted_sky_response,
        measured_correlation,
        keep_indicator,
        tile_owner[:, 0],
        tile_channel,
        tile_base,
        pairs,
        all_gains.reshape(-1, directions, LANES),
        half,
        sub_count,
    )
    outputs = finish(
        rho,
        packed.reshape((chan_count, sub_count) + packed.shape[1:]),
        jnp.swapaxes(duals, 2, 3),
        jnp.swapaxes(consensus, 2, 3),
        chan_count,
        sub_count,
    )
    return tuple(jnp.swapaxes(x, 2, 3) for x in outputs)


def solution(mesh):
    placed = (
        P(("groups", "chan", "sub"), None, None, None),
        P(("groups", "chan", "sub"), None, None),
        P(("groups", "chan", "sub"), None),
        P(("groups", "chan", "sub"), None),
        P(("groups", "chan", "sub")),
        P(("groups", "chan", "sub")),
        P(),
        P(("groups", "chan"), None, None, None),
        P(("groups", "chan", "sub"), None, None, None),
        P("groups", None, None, None),
        P(),
    )
    return jax.shard_map(
        body,
        mesh=mesh,
        in_specs=placed,
        out_specs=(
            P(("groups", "chan", "sub"), None, None, None),
            P("groups", None, None, None),
            P(("groups", "chan", "sub"), None, None, None),
        ),
        check_vma=False,
    )
```
